32 devices in a mesh: dp: 4 (over y, core), mp: 8 (over z, x).
Axes of the slice: x: 2, y: 2, z: 4, core: 2. Of those that a mesh axis runs over, the one named last changes fastest.
Arguments:
- emb_grad: float32 [65536, 7168], P('dp', 'mp'), may hold values from -600 to 600
- mtp_grad: float32 [14336, 7168], P('dp', 'mp'), may hold values from -600 to 600
- emb_groups: int32 [64], replicated, may hold values from 0 to 31
- mtp_groups: int32 [32], replicated, may hold values from 0 to 31
- max_rms: float32 [1], replicated, may hold values from 0.5 to 2
Outputs:
- emb_clipped: bfloat16 [65536, 7168], P(('dp', 'mp'))
- mtp_clipped: bfloat16 [14336, 7168], P('dp', 'mp')
- group_rms: float32 [32], replicated
The draws below stay inside these ranges and needn't reach their ends.
All inputs are finite; a program needn't handle non-finite values.
Results may differ from the reference program's by a relative error of at most 0.005.
Values may be sent and summed in bfloat16 or wider, within the bound.
A program may use at most 192 MiB of HBM per device.

```python
import math
import jax
import jax.numpy as jnp
from jax import lax

D = 7168
V = 65536
CAT = 14336
EMB_BLK = 1024
MTP_BLK = 448
GROUPS = 32
EMB_BLOCKS = 64
MTP_BLOCKS = 32


def scaled_gradient(key, height, breadth):
    keys = jax.random.split(key, 3)
    row_pos = jnp.arange(height, dtype=jnp.float32) / height
    col_pos = jnp.arange(breadth, dtype=jnp.float32) / breadth
    lower, upper = (math.log(0.3), math.log(3.0))
    base = jnp.clip(jax.random.normal(keys[0], (height, breadth), jnp.float32), -6.0, 6.0)
    row_scale = 3.0 ** (1.0 - row_pos) * jnp.exp(jax.random.uniform(keys[1], (height,), jnp.float32, lower, upper))
    col_scale = 1.8 ** col_pos * jnp.exp(jax.random.uniform(keys[2], (breadth,), jnp.float32, lower, upper))
    return base * row_scale[:, None] * col_scale[None, :]


def draw_emb_grad(key, part):
    return scaled_gradient(jax.random.fold_in(key, 11), V, D)


def draw_mtp_grad(key, part):
    return scaled_gradient(jax.random.fold_in(key, 23), CAT, D)


def with_ends(result, rng, low, largest):
    dims = result.shape
    index_at = [jax.random.randint(jax.random.fold_in(rng, axis), (), 0, dims[axis]) for axis in range(len(dims))]
    result = result.at[tuple(index_at)].set(low)
    longest = dims.index(max(dims))
    index_at[longest] = (index_at[longest] + 1) % dims[longest]
    return result.at[tuple(index_at)].set(largest)


def setup_inputs(seed: int = 0) -> dict:
    key_of = jax.random.split(jax.random.key(seed), 6)
    emb_grad = draw_emb_grad(jax.random.fold_in(key_of[5], 71), 0)
    mtp_grad = draw_mtp_grad(jax.random.fold_in(key_of[5], 71), 0)
    emb_groups = with_ends(jax.random.randint(key_of[2], (EMB_BLOCKS,), 0, GROUPS), jax.random.fold_in(key_of[2], 1), 0, GROUPS - 1).astype(jnp.int32)
    mtp_groups = with_ends(jax.random.randint(key_of[3], (MTP_BLOCKS,), 0, GROUPS), jax.random.fold_in(key_of[3], 1), 0, GROUPS - 1).astype(jnp.int32)
    max_rms = jnp.clip(jnp.exp(jax.random.uniform(key_of[4], (1,), jnp.float32, math.log(0.5), math.log(2.0))), 0.5, 2.0)
    return dict(emb_grad=emb_grad, mtp_grad=mtp_grad, emb_groups=emb_groups, mtp_groups=mtp_groups, max_rms=max_rms)


def block_squares(gradient, block_rows):
    blocks = gradient.reshape(gradient.shape[0] // block_rows, block_rows, gradient.shape[1])
    return lax.optimization_barrier(jnp.sum(jnp.square(blocks), axis=(1, 2)))

def membership(labels):
    return (labels[:, None] == jnp.arange(GROUPS, dtype=jnp.int32)[None, :]).astype(jnp.float32)

def reference(emb_grad, mtp_grad, emb_groups, mtp_groups, max_rms):
    embed_member = membership(emb_groups)
    head_member = membership(mtp_groups)
    embed_squares = block_squares(emb_grad, EMB_BLK)
    head_squares = block_squares(mtp_grad, MTP_BLK)
    group_square = lax.optimization_barrier(jnp.sum(embed_squares[:, None] * embed_member, axis=0)) + lax.optimization_barrier(jnp.sum(head_squares[:, None] * head_member, axis=0))
    group_size = lax.optimization_barrier(jnp.sum(embed_member, axis=0)) * jnp.float32(EMB_BLK * D) + lax.optimization_barrier(jnp.sum(head_member, axis=0)) * jnp.float32(MTP_BLK * D)
    group_rms = jnp.sqrt(group_square / jnp.maximum(group_size, 1.0))
    global_norm = jnp.sqrt(jnp.sum(group_square))
    ceiling = max_rms[0] * jnp.sqrt(jnp.float32((V + CAT) * D))
    factor = ceiling / (global_norm + 1e-06)
    emb_low = lax.optimization_barrier(emb_grad.astype(jnp.bfloat16))
    emb_clipped = (emb_low.astype(jnp.float32) * factor).astype(jnp.bfloat16)
    mtp_clipped = (mtp_grad * factor).astype(jnp.bfloat16)
    return (emb_clipped, mtp_clipped, group_rms)
```

```python
import functools

import jax
import jax.numpy as jnp
from jax import lax
from jax.experimental import pallas as pl
from jax.experimental.pallas import tpu as pltpu
from jax.sharding import PartitionSpec as P

EMB_BLK = 1024
MTP_BLK = 448
GROUPS = 32
STRIP = 32
SLOTS = 6
LANES = 128
MESH = pl.DeviceIdType.MESH


def partner(me, k, count):
    out, bit = 0, 1
    while bit < count:
        mine, other = (me // bit) % 2, (k // bit) % 2
        out = out + bit * (mine + other - 2 * mine * other)
        bit *= 2
    return out


def exchange_kernel(
    pieces, shards, tiles, tail_tiles,
    emb, mtp, arrived, tail_out, sums,
    low, tail, slots, head_slots, squares, mine, column_sums, shard_mine, shard_sums,
    load_sem, head_sem, send_sem, recv_sem, own_sem, tail_sem,
    stat_send, stat_recv, shard_send, shard_recv,
):
    me, shard = lax.axis_index("mp"), lax.axis_index("dp")
    _, rows, width = emb.shape
    tile = slots.shape[1]
    embed_blocks = pieces * rows // EMB_BLK
    head_blocks = mtp.shape[0] // MTP_BLK
    bulk = tiles - tail_tiles
    half = bulk // 2

    barrier = pltpu.get_barrier_semaphore()
    for k in range(1, pieces):
        pl.semaphore_signal(
            barrier, inc=1, device_id={"mp": partner(me, k, pieces)}, device_id_type=MESH
        )
    for k in range(1, shards):
        pl.semaphore_signal(
            barrier, inc=1, device_id={"dp": partner(shard, k, shards)}, device_id_type=MESH
        )

    squares[...] = jnp.zeros_like(squares)

    def stream(count, place, work, after):
        def load(i):
            piece, t = place(i)
            return pltpu.make_async_copy(
                emb.at[piece, pl.ds(pl.multiple_of(t * tile, tile), tile), :],
                slots.at[i % SLOTS],
                load_sem.at[i % SLOTS],
            )

        def prime():
            for i in range(min(SLOTS, count)):
                load(i).start()

        def run():
            @pl.loop(0, count)
            def _(i):
                load(i).wait()
                piece, t = place(i)
                block = (piece * rows + t * tile) // EMB_BLK
                target = work(i)
                slot = i % SLOTS

                def strip(j, total):
                    at = pl.multiple_of(j * STRIP, STRIP)
                    x = slots[slot, pl.ds(at, STRIP), :]
                    target(at, x.astype(jnp.bfloat16))
                    return total + jnp.sum((x * x).reshape(STRIP // 8, 8, width), axis=0)

                total = lax.fori_loop(
                    0, tile // STRIP, strip, jnp.zeros((8, width), jnp.float32)
                )
                squares[block] = squares[block] + total

                @pl.when(i + SLOTS < count)
                def _():
                    load(i + SLOTS).start()

                @pl.when(i > 0)
                def _():
                    after(i - 1)

            after(count - 1)

        return prime, run

    def send(k, t):
        at = pl.ds(pl.multiple_of(t * tile, tile), tile)
        return pltpu.make_async_remote_copy(
            src_ref=low.at[k, at, :],
            dst_ref=arrived.at[me, at, :],
            send_sem=send_sem.at[k],
            recv_sem=recv_sem.at[k],
            device_id={"mp": partner(me, k, pieces)},
            device_id_type=MESH,
        )

    others = pieces - 1

    def group_of(i):
        return 1 + (i + 1) % others

    def store_low(k, t):
        def target(at, value):
            low[k, pl.ds(pl.multiple_of(t * tile + at, STRIP), STRIP), :] = value

        return target

    first_prime, first_run = stream(
        others,
        lambda i: (partner(me, group_of(i), pieces), 0),
        lambda i: store_low(group_of(i), 0),
        lambda i: send(group_of(i), 0).start(),
    )
    first_prime()
    pl.semaphore_wait(barrier, pieces - 1 + shards - 1)
    first_run()

    rest = bulk - 1

    def rest_after(i):
        k, t = group_of(i // rest), 1 + i % rest

        @pl.when((k < pieces // 2) | (t < half))
        def _():
            send(k, t).start()

    rest_prime, rest_run = stream(
        others * rest,
        lambda i: (partner(me, group_of(i // rest), pieces), 1 + i % rest),
        lambda i: store_low(group_of(i // rest), 1 + i % rest),
        rest_after,
    )
    rest_prime()
    rest_run()

    def own_copy(t):
        at = pl.ds(pl.multiple_of(t * tile, tile), tile)
        return pltpu.make_async_copy(low.at[0, at, :], arrived.at[me, at, :], own_sem)

    own_prime, own_run = stream(
        bulk, lambda i: (me, i), lambda i: store_low(0, i), lambda i: own_copy(i).start()
    )
    own_prime()
    own_run()

    def store_tail(i):
        def target(at, value):
            row = pl.multiple_of((i % tail_tiles) * tile + at, STRIP)
            tail[i // tail_tiles, pl.ds(row, STRIP), :] = value

        return target

    def tail_copy(i):
        at = pl.ds(pl.multiple_of((i % tail_tiles) * tile, tile), tile)
        piece = i // tail_tiles
        return pltpu.make_async_copy(
            tail.at[piece, at, :], tail_out.at[piece, at, :], tail_sem
        )

    tail_prime, tail_run = stream(
        pieces * tail_tiles,
        lambda i: (i // tail_tiles, bulk + i % tail_tiles),
        store_tail,
        lambda i: tail_copy(i).start(),
    )
    tail_prime()
    tail_run()

    def head_load(b):
        return pltpu.make_async_copy(
            mtp.at[pl.ds(pl.multiple_of(b * MTP_BLK, MTP_BLK), MTP_BLK), :],
            head_slots.at[b % 2],
            head_sem.at[b % 2],
        )

    for b in range(min(2, head_blocks)):
        head_load(b).start()

    @pl.loop(0, head_blocks)
    def _(b):
        head_load(b).wait()

        def strip(j, total):
            x = head_slots[b % 2, pl.ds(pl.multiple_of(j * STRIP, STRIP), STRIP), :]
            return total + jnp.sum((x * x).reshape(STRIP // 8, 8, width), axis=0)

        squares[embed_blocks + b] = lax.fori_loop(
            0, MTP_BLK // STRIP, strip, jnp.zeros((8, width), jnp.float32)
        )

        @pl.when(b + 2 < head_blocks)
        def _():
            head_load(b + 2).start()

    lane = lax.broadcasted_iota(jnp.int32, (8, LANES), 0) * LANES + lax.broadcasted_iota(
        jnp.int32, (8, LANES), 1
    )

    def pack(b, total):
        return jnp.where(lane == b, jnp.sum(squares[b]), total)

    packed = lax.fori_loop(
        0, embed_blocks + head_blocks, pack, jnp.zeros((8, LANES), jnp.float32)
    )
    mine[...] = packed
    column_sums[me] = packed

    def far_sends(low_tile, high_tile):
        span = high_tile - low_tile

        @pl.loop(0, (pieces - pieces // 2) * span)
        def _(i):
            send(pieces // 2 + i // span, low_tile + i % span).start()

    split = half + (bulk - half) // 2
    far_sends(half, split)

    def stat_copy(k):
        return pltpu.make_async_remote_copy(
            src_ref=mine,
            dst_ref=column_sums.at[me],
            send_sem=stat_send.at[k],
            recv_sem=stat_recv.at[k],
            device_id={"mp": partner(me, k, pieces)},
            device_id_type=MESH,
        )

    for k in range(1, pieces):
        stat_copy(k).start()
    far_sends(split, bulk)
    for k in range(1, pieces):
        stat_copy(k).wait()
    packed = jnp.sum(column_sums[...], axis=0)
    shard_mine[...] = packed
    shard_sums[shard] = packed

    def whole_copy(k):
        at = pl.ds(0, bulk * tile)
        return pltpu.make_async_remote_copy(
            src_ref=low.at[k, at, :],
            dst_ref=arrived.at[me, at, :],
            send_sem=send_sem.at[k],
            recv_sem=recv_sem.at[k],
            device_id={"mp": partner(me, k, pieces)},
            device_id_type=MESH,
        )

    whole_copy(1).wait_send()

    def shard_copy(k):
        return pltpu.make_async_remote_copy(
            src_ref=shard_mine,
            dst_ref=shard_sums.at[shard],
            send_sem=shard_send.at[k],
            recv_sem=shard_recv.at[k],
            device_id={"dp": partner(shard, k, shards)},
            device_id_type=MESH,
        )

    for k in range(1, shards):
        shard_copy(k).start()
    for k in range(1, shards):
        shard_copy(k).wait()
    sums[...] = shard_sums[...]

    at = pl.ds(0, bulk * tile)
    pltpu.make_async_copy(low.at[0, at, :], arrived.at[me, at, :], own_sem).wait()
    pltpu.make_async_copy(tail, tail_out, tail_sem).wait()
    whole_copy(1).wait_recv()
    for k in range(2, pieces):
        whole_copy(k).wait()


def round_and_exchange(by_owner, mtp, shards, tiles, tail_tiles):
    pieces, rows, width = by_owner.shape
    tile = rows // tiles
    bulk_rows, tail_rows = (tiles - tail_tiles) * tile, tail_tiles * tile
    blocks = pieces * rows // EMB_BLK + mtp.shape[0] // MTP_BLK
    return pl.pallas_call(
        functools.partial(exchange_kernel, pieces, shards, tiles, tail_tiles),
        in_specs=[pl.BlockSpec(memory_space=pl.ANY)] * 2,
        out_specs=[
            pl.BlockSpec(memory_space=pl.ANY),
            pl.BlockSpec(memory_space=pl.ANY),
            pl.BlockSpec(memory_space=pltpu.VMEM),
        ],
        out_shape=[
            jax.ShapeDtypeStruct((pieces, bulk_rows, width), jnp.bfloat16),
            jax.ShapeDtypeStruct((pieces, tail_rows, width), jnp.bfloat16),
            jax.ShapeDtypeStruct((shards, 8, LANES), jnp.float32),
        ],
        scratch_shapes=[
            pltpu.VMEM((pieces, bulk_rows, width), jnp.bfloat16),
            pltpu.VMEM((pieces, tail_rows, width), jnp.bfloat16),
            pltpu.VMEM((SLOTS, tile, width), jnp.float32),
            pltpu.VMEM((2, MTP_BLK, width), jnp.float32),
            pltpu.VMEM((blocks, 8, width), jnp.float32),
            pltpu.VMEM((8, LANES), jnp.float32),
            pltpu.VMEM((pieces, 8, LANES), jnp.float32),
            pltpu.VMEM((8, LANES), jnp.float32),
            pltpu.VMEM((shards, 8, LANES), jnp.float32),
            pltpu.SemaphoreType.DMA((SLOTS,)),
            pltpu.SemaphoreType.DMA((2,)),
            pltpu.SemaphoreType.DMA((pieces,)),
            pltpu.SemaphoreType.DMA((pieces,)),
            pltpu.SemaphoreType.DMA,
            pltpu.SemaphoreType.DMA,
            pltpu.SemaphoreType.DMA((pieces,)),
            pltpu.SemaphoreType.DMA((pieces,)),
            pltpu.SemaphoreType.DMA((shards,)),
            pltpu.SemaphoreType.DMA((shards,)),
        ],
        compiler_params=pltpu.CompilerParams(
            collective_id=0, has_side_effects=True, vmem_limit_bytes=60_000_000
        ),
        cost_estimate=pl.CostEstimate(
            flops=3 * by_owner.size, bytes_accessed=8 * by_owner.size, transcendentals=0
        ),
    )(by_owner, mtp)


def scale_kernel(factor_ref, x_ref, *refs):
    out_ref = refs[-1]
    pieces, _, width = x_ref.shape
    factor = factor_ref[0]
    for j in range(pieces):
        out_ref[:, j * width : (j + 1) * width] = (
            x_ref[j].astype(jnp.float32) * factor
        ).astype(jnp.bfloat16)


def scale_rows(factor, arrived, out, first, rows, tile):
    pieces, count, width = arrived.shape
    start = first // tile
    in_specs = [
        pl.BlockSpec(memory_space=pltpu.SMEM),
        pl.BlockSpec((pieces, tile, width), lambda i: (0, i, 0)),
    ]
    operands = [factor.reshape(1), arrived]
    aliases = {}
    if out is not None:
        in_specs.append(pl.BlockSpec(memory_space=pl.ANY))
        operands.append(out)
        aliases = {2: 0}
    return pl.pallas_call(
        scale_kernel,
        grid=(count // tile,),
        in_specs=in_specs,
        out_specs=pl.BlockSpec((tile, pieces * width), lambda i: (start + i, 0)),
        out_shape=jax.ShapeDtypeStruct((rows, pieces * width), jnp.bfloat16),
        input_output_aliases=aliases,
        cost_estimate=pl.CostEstimate(
            flops=arrived.size, bytes_accessed=4 * arrived.size, transcendentals=0
        ),
    )(*operands)


def membership(labels):
    return (labels[:, None] == jnp.arange(GROUPS, dtype=jnp.int32)[None, :]).astype(jnp.float32)


def on_device(shards, pieces, emb_grad, mtp_grad, emb_groups, mtp_groups, max_rms):
    width = emb_grad.shape[1]
    model_width = width * pieces
    total_rows = (emb_grad.shape[0] + mtp_grad.shape[0]) * shards
    rows = emb_grad.shape[0] // pieces
    tiles, tail_tiles = 16, 1
    tile = rows // tiles
    bulk_rows = (tiles - tail_tiles) * tile

    by_owner = emb_grad.reshape(pieces, rows, width)
    arrived, tail, sums = round_and_exchange(by_owner, mtp_grad, shards, tiles, tail_tiles)
    tail_arrived = lax.all_to_all(tail, "mp", split_axis=0, concat_axis=0, tiled=True)

    embed_count = emb_grad.shape[0] // EMB_BLK
    head_count = mtp_grad.shape[0] // MTP_BLK
    flat = sums.reshape(shards, 8 * LANES)
    embed_squares = flat[:, :embed_count].reshape(-1)
    head_squares = flat[:, embed_count : embed_count + head_count].reshape(-1)
    embed_member, head_member = membership(emb_groups), membership(mtp_groups)
    group_square = jnp.sum(embed_squares[:, None] * embed_member, axis=0) + jnp.sum(
        head_squares[:, None] * head_member, axis=0
    )
    group_size = jnp.sum(embed_member, axis=0) * jnp.float32(
        EMB_BLK * model_width
    ) + jnp.sum(head_member, axis=0) * jnp.float32(MTP_BLK * model_width)
    group_rms = jnp.sqrt(group_square / jnp.maximum(group_size, 1.0))
    global_norm = jnp.sqrt(jnp.sum(group_square))
    ceiling = max_rms[0] * jnp.sqrt(jnp.float32(total_rows * model_width))
    factor = ceiling / (global_norm + 1e-06)
    out = scale_rows(factor, arrived, None, 0, rows, tile)
    head_output = (mtp_grad * factor).astype(jnp.bfloat16)
    out = scale_rows(factor, tail_arrived, out, bulk_rows, rows, tile)
    return (out, head_output, group_rms)


def solution(mesh):
    placed = (P("dp", "mp"), P("dp", "mp"), P(), P(), P())
    return jax.shard_map(
        functools.partial(on_device, mesh.shape["dp"], mesh.shape["mp"]),
        mesh=mesh,
        in_specs=placed,
        out_specs=(P(("dp", "mp"), None), P("dp", "mp"), P()),
        check_vma=False,
    )
```

```python
import functools

import jax
import jax.numpy as jnp
from jax import lax
from jax.experimental import pallas as pl
from jax.experimental.pallas import tpu as pltpu
from jax.sharding import PartitionSpec as P

EMB_BLK = 1024
MTP_BLK = 448
GROUPS = 32
STRIP = 32
SLOTS = 6
LEAD = 2
LANES = 128
MESH = pl.DeviceIdType.MESH


def partner(me, k, count):
    out, bit = 0, 1
    while bit < count:
        mine, other = (me // bit) % 2, (k // bit) % 2
        out = out + bit * (mine + other - 2 * mine * other)
        bit *= 2
    return out


def exchange_kernel(
    pieces, shards, tiles, tail_tiles,
    emb, mtp, arrived, tail_out, sums,
    low, tail, slots, head_slots, squares, mine, column_sums, shard_mine, shard_sums,
    load_sem, head_sem, send_sem, recv_sem, own_sem, tail_sem,
    stat_send, stat_recv, shard_send, shard_recv,
):
    me, shard = lax.axis_index("mp"), lax.axis_index("dp")
    _, rows, width = emb.shape
    tile = slots.shape[1]
    embed_blocks = pieces * rows // EMB_BLK
    head_blocks = mtp.shape[0] // MTP_BLK
    bulk = tiles - tail_tiles

    barrier = pltpu.get_barrier_semaphore()
    for k in range(1, pieces):
        pl.semaphore_signal(
            barrier, inc=1, device_id={"mp": partner(me, k, pieces)}, device_id_type=MESH
        )
    for k in range(1, shards):
        pl.semaphore_signal(
            barrier, inc=1, device_id={"dp": partner(shard, k, shards)}, device_id_type=MESH
        )

    squares[...] = jnp.zeros_like(squares)

    def stream(count, place, store, after):
        def load(i):
            piece, t = place(i)
            return pltpu.make_async_copy(
                emb.at[piece, pl.ds(pl.multiple_of(t * tile, tile), tile), :],
                slots.at[i % SLOTS],
                load_sem.at[i % SLOTS],
            )

        def prime():
            for i in range(min(SLOTS, count)):
                load(i).start()

        def run():
            @pl.loop(0, count)
            def _(i):
                load(i).wait()
                piece, t = place(i)
                block = (piece * rows + t * tile) // EMB_BLK
                slot = i % SLOTS

                def strip(j, total):
                    at = pl.multiple_of(j * STRIP, STRIP)
                    x = slots[slot, pl.ds(at, STRIP), :]
                    store(i, at, x.astype(jnp.bfloat16))
                    return total + jnp.sum((x * x).reshape(STRIP // 8, 8, width), axis=0)

                total = lax.fori_loop(
                    0, tile // STRIP, strip, jnp.zeros((8, width), jnp.float32)
                )
                squares[block] = squares[block] + total

                @pl.when(i + SLOTS < count)
                def _():
                    load(i + SLOTS).start()

                @pl.when(i > 0)
                def _():
                    after(i - 1)

            after(count - 1)

        return prime, run

    def store_low(k, t, at, value):
        low[k, pl.ds(pl.multiple_of(t * tile + at, STRIP), STRIP), :] = value

    def send(k, start, count):
        at = pl.ds(pl.multiple_of(start * tile, tile), count * tile)
        return pltpu.make_async_remote_copy(
            src_ref=low.at[k, at, :],
            dst_ref=arrived.at[me, at, :],
            send_sem=send_sem.at[k],
            recv_sem=recv_sem.at[k],
            device_id={"mp": partner(me, k, pieces)},
            device_id_type=MESH,
        )

    middle = pieces // 2
    near = list(range(2, middle))
    early = list(range(pieces - 1, middle + middle // 2 - 1, -1))
    late = list(range(middle, middle + middle // 2))
    lead = min(LEAD, bulk - 1)
    paired = min(len(near), len(early))

    def lead_piece(i):
        pair = (i // 2) % paired
        return (1 - i % 2) * (2 + pair) + (i % 2) * (pieces - 1 - pair)

    def lead_tile(i):
        return i // (2 * paired)

    prime, run = stream(
        2 * paired * lead,
        lambda i: (partner(me, lead_piece(i), pieces), lead_tile(i)),
        lambda i, at, value: store_low(lead_piece(i), lead_tile(i), at, value),
        lambda i: send(lead_piece(i), lead_tile(i), 1).start(),
    )
    prime()
    pl.semaphore_wait(barrier, pieces - 1 + shards - 1)
    run()

    waiting = []
    for k in near + early + late + [1]:
        started = lead if k in near[:paired] + early[:paired] else 0
        prime, run = stream(
            bulk - started,
            lambda i: (partner(me, k, pieces), started + i),
            lambda i, at, value: store_low(k, started + i, at, value),
            lambda i: None,
        )
        prime()
        run()
        for copy in waiting:
            copy.start()
        waiting = [send(k, started, bulk - started)] if k in near + early else []
    first_late = late[0]
    half = bulk // 2

    own_at = pl.ds(0, bulk * tile)
    own_copy = pltpu.make_async_copy(low.at[0, own_at, :], arrived.at[me, own_at, :], own_sem)
    prime, run = stream(
        bulk,
        lambda i: (me, i),
        lambda i, at, value: store_low(0, i, at, value),
        lambda i: None,
    )
    prime()
    run()
    send(first_late, 0, half).start()

    def store_tail(i, at, value):
        row = pl.multiple_of((i % tail_tiles) * tile + at, STRIP)
        tail[i // tail_tiles, pl.ds(row, STRIP), :] = value

    tail_copy = pltpu.make_async_copy(tail, tail_out, tail_sem)
    prime, run = stream(
        pieces * tail_tiles,
        lambda i: (i // tail_tiles, bulk + i % tail_tiles),
        store_tail,
        lambda i: None,
    )
    prime()
    run()
    own_copy.start()

    def head_load(b):
        return pltpu.make_async_copy(
            mtp.at[pl.ds(pl.multiple_of(b * MTP_BLK, MTP_BLK), MTP_BLK), :],
            head_slots.at[b % 2],
            head_sem.at[b % 2],
        )

    for b in range(min(2, head_blocks)):
        head_load(b).start()

    @pl.loop(0, head_blocks)
    def _(b):
        head_load(b).wait()

        def strip(j, total):
            x = head_slots[b % 2, pl.ds(pl.multiple_of(j * STRIP, STRIP), STRIP), :]
            return total + jnp.sum((x * x).reshape(STRIP // 8, 8, width), axis=0)

        squares[embed_blocks + b] = lax.fori_loop(
            0, MTP_BLK // STRIP, strip, jnp.zeros((8, width), jnp.float32)
        )

        @pl.when(b + 2 < head_blocks)
        def _():
            head_load(b + 2).start()

    lane = lax.broadcasted_iota(jnp.int32, (8, LANES), 0) * LANES + lax.broadcasted_iota(
        jnp.int32, (8, LANES), 1
    )

    def pack(b, total):
        return jnp.where(lane == b, jnp.sum(squares[b]), total)

    packed = lax.fori_loop(
        0, embed_blocks + head_blocks, pack, jnp.zeros((8, LANES), jnp.float32)
    )
    mine[...] = packed
    column_sums[me] = packed

    tail_copy.start()

    for k in near:
        send(k, 0, bulk).wait_send()
    send(1, 0, bulk).start()

    def stat_copy(k):
        return pltpu.make_async_remote_copy(
            src_ref=mine,
            dst_ref=column_sums.at[me],
            send_sem=stat_send.at[k],
            recv_sem=stat_recv.at[k],
            device_id={"mp": partner(me, k, pieces)},
            device_id_type=MESH,
        )

    for k in range(1, pieces):
        stat_copy(k).start()
    send(first_late, half, bulk - half).start()
    for k in late[1:]:
        send(k, 0, bulk).start()
    for k in range(1, pieces):
        stat_copy(k).wait()
    packed = jnp.sum(column_sums[...], axis=0)
    shard_mine[...] = packed
    shard_sums[shard] = packed

    def shard_copy(k):
        return pltpu.make_async_remote_copy(
            src_ref=shard_mine,
            dst_ref=shard_sums.at[shard],
            send_sem=shard_send.at[k],
            recv_sem=shard_recv.at[k],
            device_id={"dp": partner(shard, k, shards)},
            device_id_type=MESH,
        )

    for k in range(1, shards):
        shard_copy(k).start()
    for k in range(1, shards):
        shard_copy(k).wait()
    sums[...] = shard_sums[...]

    own_copy.wait()
    tail_copy.wait()
    for k in range(1, pieces):
        if k not in near:
            send(k, 0, bulk).wait_send()
        send(k, 0, bulk).wait_recv()


def round_and_exchange(by_owner, mtp, shards, tiles, tail_tiles):
    pieces, rows, width = by_owner.shape
    tile = rows // tiles
    bulk_rows, tail_rows = (tiles - tail_tiles) * tile, tail_tiles * tile
    blocks = pieces * rows // EMB_BLK + mtp.shape[0] // MTP_BLK
    return pl.pallas_call(
        functools.partial(exchange_kernel, pieces, shards, tiles, tail_tiles),
        in_specs=[pl.BlockSpec(memory_space=pl.ANY)] * 2,
        out_specs=[
            pl.BlockSpec(memory_space=pl.ANY),
            pl.BlockSpec(memory_space=pl.ANY),
            pl.BlockSpec(memory_space=pltpu.VMEM),
        ],
        out_shape=[
            jax.ShapeDtypeStruct((pieces, bulk_rows, width), jnp.bfloat16),
            jax.ShapeDtypeStruct((pieces, tail_rows, width), jnp.bfloat16),
            jax.ShapeDtypeStruct((shards, 8, LANES), jnp.float32),
        ],
        scratch_shapes=[
            pltpu.VMEM((pieces, bulk_rows, width), jnp.bfloat16),
            pltpu.VMEM((pieces, tail_rows, width), jnp.bfloat16),
            pltpu.VMEM((SLOTS, tile, width), jnp.float32),
            pltpu.VMEM((2, MTP_BLK, width), jnp.float32),
            pltpu.VMEM((blocks, 8, width), jnp.float32),
            pltpu.VMEM((8, LANES), jnp.float32),
            pltpu.VMEM((pieces, 8, LANES), jnp.float32),
            pltpu.VMEM((8, LANES), jnp.float32),
            pltpu.VMEM((shards, 8, LANES), jnp.float32),
            pltpu.SemaphoreType.DMA((SLOTS,)),
            pltpu.SemaphoreType.DMA((2,)),
            pltpu.SemaphoreType.DMA((pieces,)),
            pltpu.SemaphoreType.DMA((pieces,)),
            pltpu.SemaphoreType.DMA,
            pltpu.SemaphoreType.DMA,
            pltpu.SemaphoreType.DMA((pieces,)),
            pltpu.SemaphoreType.DMA((pieces,)),
            pltpu.SemaphoreType.DMA((shards,)),
            pltpu.SemaphoreType.DMA((shards,)),
        ],
        compiler_params=pltpu.CompilerParams(
            collective_id=0, has_side_effects=True, vmem_limit_bytes=60_000_000
        ),
        cost_estimate=pl.CostEstimate(
            flops=3 * by_owner.size, bytes_accessed=8 * by_owner.size, transcendentals=0
        ),
    )(by_owner, mtp)


def scale_kernel(factor_ref, x_ref, *refs):
    out_ref = refs[-1]
    pieces, _, width = x_ref.shape
    factor = factor_ref[0]
    for j in range(pieces):
        out_ref[:, j * width : (j + 1) * width] = (
            x_ref[j].astype(jnp.float32) * factor
        ).astype(jnp.bfloat16)


def scale_rows(factor, arrived, out, first, rows, tile):
    pieces, count, width = arrived.shape
    start = first // tile
    in_specs = [
        pl.BlockSpec(memory_space=pltpu.SMEM),
        pl.BlockSpec((pieces, tile, width), lambda i: (0, i, 0)),
    ]
    operands = [factor.reshape(1), arrived]
    aliases = {}
    if out is not None:
        in_specs.append(pl.BlockSpec(memory_space=pl.ANY))
        operands.append(out)
        aliases = {2: 0}
    return pl.pallas_call(
        scale_kernel,
        grid=(count // tile,),
        in_specs=in_specs,
        out_specs=pl.BlockSpec((tile, pieces * width), lambda i: (start + i, 0)),
        out_shape=jax.ShapeDtypeStruct((rows, pieces * width), jnp.bfloat16),
        input_output_aliases=aliases,
        cost_estimate=pl.CostEstimate(
            flops=arrived.size, bytes_accessed=4 * arrived.size, transcendentals=0
        ),
    )(*operands)


def membership(labels):
    return (labels[:, None] == jnp.arange(GROUPS, dtype=jnp.int32)[None, :]).astype(jnp.float32)


def on_device(shards, pieces, emb_grad, mtp_grad, emb_groups, mtp_groups, max_rms):
    width = emb_grad.shape[1]
    model_width = width * pieces
    total_rows = (emb_grad.shape[0] + mtp_grad.shape[0]) * shards
    rows = emb_grad.shape[0] // pieces
    tiles, tail_tiles = 16, 1
    tile = rows // tiles
    bulk_rows = (tiles - tail_tiles) * tile

    by_owner = emb_grad.reshape(pieces, rows, width)
    arrived, tail, sums = round_and_exchange(by_owner, mtp_grad, shards, tiles, tail_tiles)
    tail_arrived = lax.all_to_all(tail, "mp", split_axis=0, concat_axis=0, tiled=True)

    embed_count = emb_grad.shape[0] // EMB_BLK
    head_count = mtp_grad.shape[0] // MTP_BLK
    flat = sums.reshape(shards, 8 * LANES)
    embed_squares = flat[:, :embed_count].reshape(-1)
    head_squares = flat[:, embed_count : embed_count + head_count].reshape(-1)
    embed_member, head_member = membership(emb_groups), membership(mtp_groups)
    group_square = jnp.sum(embed_squares[:, None] * embed_member, axis=0) + jnp.sum(
        head_squares[:, None] * head_member, axis=0
    )
    group_size = jnp.sum(embed_member, axis=0) * jnp.float32(
        EMB_BLK * model_width
    ) + jnp.sum(head_member, axis=0) * jnp.float32(MTP_BLK * model_width)
    group_rms = jnp.sqrt(group_square / jnp.maximum(group_size, 1.0))
    global_norm = jnp.sqrt(jnp.sum(group_square))
    ceiling = max_rms[0] * jnp.sqrt(jnp.float32(total_rows * model_width))
    factor = ceiling / (global_norm + 1e-06)
    out = scale_rows(factor, arrived, None, 0, rows, tile)
    head_output = (mtp_grad * factor).astype(jnp.bfloat16)
    out = scale_rows(factor, tail_arrived, out, bulk_rows, rows, tile)
    return (out, head_output, group_rms)


def solution(mesh):
    placed = (P("dp", "mp"), P("dp", "mp"), P(), P(), P())
    return jax.shard_map(
        functools.partial(on_device, mesh.shape["dp"], mesh.shape["mp"]),
        mesh=mesh,
        in_specs=placed,
        out_specs=(P(("dp", "mp"), None), P("dp", "mp"), P()),
        check_vma=False,
    )
```

```python
import functools

import jax
import jax.numpy as jnp
from jax import lax
from jax.experimental import pallas as pl
from jax.experimental.pallas import tpu as pltpu
from jax.sharding import PartitionSpec as P

EMB_BLK = 1024
MTP_BLK = 448
GROUPS = 32
STRIP = 32
SLOTS = 6
LEAD = 2
LANES = 128
MESH = pl.DeviceIdType.MESH


def partner(me, k, count):
    out, bit = 0, 1
    while bit < count:
        mine, other = (me // bit) % 2, (k // bit) % 2
        out = out + bit * (mine + other - 2 * mine * other)
        bit *= 2
    return out


def exchange_kernel(
    pieces, shards, tiles, tail_tiles,
    emb, mtp, arrived, tail_out, sums,
    low, tail, slots, head_slots, squares, mine, column_sums, shard_mine, shard_sums,
    load_sem, head_sem, send_sem, recv_sem, own_sem, tail_sem,
    stat_send, stat_recv, shard_send, shard_recv,
):
    me, shard = lax.axis_index("mp"), lax.axis_index("dp")
    _, rows, width = emb.shape
    tile = slots.shape[1]
    embed_blocks = pieces * rows // EMB_BLK
    head_blocks = mtp.shape[0] // MTP_BLK
    bulk = tiles - tail_tiles

    barrier = pltpu.get_barrier_semaphore()
    for k in range(1, pieces):
        pl.semaphore_signal(
            barrier, inc=1, device_id={"mp": partner(me, k, pieces)}, device_id_type=MESH
        )
    for k in range(1, shards):
        pl.semaphore_signal(
            barrier, inc=1, device_id={"dp": partner(shard, k, shards)}, device_id_type=MESH
        )

    def stream(count, place, store, after):
        def load(i):
            piece, t = place(i)
            return pltpu.make_async_copy(
                emb.at[piece, pl.ds(pl.multiple_of(t * tile, tile), tile), :],
                slots.at[i % SLOTS],
                load_sem.at[i % SLOTS],
            )

        def prime():
            for i in range(min(SLOTS, count)):
                load(i).start()

        def run():
            @pl.loop(0, count)
            def _(i):
                load(i).wait()
                piece, t = place(i)
                block = (piece * rows + t * tile) // EMB_BLK
                slot = i % SLOTS

                def strip(j, total):
                    at = pl.multiple_of(j * STRIP, STRIP)
                    x = slots[slot, pl.ds(at, STRIP), :]
                    store(i, at, x.astype(jnp.bfloat16))
                    return total + jnp.sum((x * x).reshape(STRIP // 8, 8, width), axis=0)

                total = lax.fori_loop(
                    0, tile // STRIP, strip, jnp.zeros((8, width), jnp.float32)
                )
                squares[block] = squares[block] + total

                @pl.when(i + SLOTS < count)
                def _():
                    load(i + SLOTS).start()

                @pl.when(i > 0)
                def _():
                    after(i - 1)

            after(count - 1)

        return prime, run

    def store_low(k, t, at, value):
        low[k, pl.ds(pl.multiple_of(t * tile + at, STRIP), STRIP), :] = value

    def send(k, start, count):
        at = pl.ds(pl.multiple_of(start * tile, tile), count * tile)
        return pltpu.make_async_remote_copy(
            src_ref=low.at[k, at, :],
            dst_ref=arrived.at[me, at, :],
            send_sem=send_sem.at[k],
            recv_sem=recv_sem.at[k],
            device_id={"mp": partner(me, k, pieces)},
            device_id_type=MESH,
        )

    middle = pieces // 2
    near = list(range(2, middle))
    early = list(range(pieces - 1, middle + middle // 2 - 1, -1))
    late = list(range(middle + middle // 2 - 1, middle - 1, -1))
    lead = min(LEAD, bulk - 1)
    paired = min(len(near), len(early))

    def lead_piece(i):
        pair = (i // 2) % paired
        return (1 - i % 2) * (2 + pair) + (i % 2) * (pieces - 1 - pair)

    def lead_tile(i):
        return i // (2 * paired)

    prime, run = stream(
        2 * paired * lead,
        lambda i: (partner(me, lead_piece(i), pieces), lead_tile(i)),
        lambda i, at, value: store_low(lead_piece(i), lead_tile(i), at, value),
        lambda i: None,
    )
    prime()
    squares[...] = jnp.zeros_like(squares)
    run()
    pl.semaphore_wait(barrier, pieces - 1 + shards - 1)
    for pair in range(paired):
        send(near[pair], 0, lead).start()
        send(early[pair], 0, lead).start()

    waiting = []
    for k in near + early + late + [1]:
        started = lead if k in near[:paired] + early[:paired] else 0
        prime, run = stream(
            bulk - started,
            lambda i: (partner(me, k, pieces), started + i),
            lambda i, at, value: store_low(k, started + i, at, value),
            lambda i: None,
        )
        prime()
        run()
        for copy in waiting:
            copy.start()
        waiting = [send(k, started, bulk - started)] if k in near + early else []
    first_late = late[0]
    half = bulk // 2

    own_at = pl.ds(0, bulk * tile)
    own_copy = pltpu.make_async_copy(low.at[0, own_at, :], arrived.at[me, own_at, :], own_sem)
    prime, run = stream(
        bulk,
        lambda i: (me, i),
        lambda i, at, value: store_low(0, i, at, value),
        lambda i: None,
    )
    prime()
    run()
    send(first_late, 0, half).start()

    def store_tail(i, at, value):
        row = pl.multiple_of((i % tail_tiles) * tile + at, STRIP)
        tail[i // tail_tiles, pl.ds(row, STRIP), :] = value

    tail_copy = pltpu.make_async_copy(tail, tail_out, tail_sem)
    prime, run = stream(
        pieces * tail_tiles,
        lambda i: (i // tail_tiles, bulk + i % tail_tiles),
        store_tail,
        lambda i: None,
    )
    prime()
    run()
    own_copy.start()

    def head_load(b):
        return pltpu.make_async_copy(
            mtp.at[pl.ds(pl.multiple_of(b * MTP_BLK, MTP_BLK), MTP_BLK), :],
            head_slots.at[b % 2],
            head_sem.at[b % 2],
        )

    for b in range(min(2, head_blocks)):
        head_load(b).start()

    @pl.loop(0, head_blocks)
    def _(b):
        head_load(b).wait()

        def strip(j, total):
            x = head_slots[b % 2, pl.ds(pl.multiple_of(j * STRIP, STRIP), STRIP), :]
            return total + jnp.sum((x * x).reshape(STRIP // 8, 8, width), axis=0)

        squares[embed_blocks + b] = lax.fori_loop(
            0, MTP_BLK // STRIP, strip, jnp.zeros((8, width), jnp.float32)
        )

        @pl.when(b + 2 < head_blocks)
        def _():
            head_load(b + 2).start()

    lane = lax.broadcasted_iota(jnp.int32, (8, LANES), 0) * LANES + lax.broadcasted_iota(
        jnp.int32, (8, LANES), 1
    )

    def pack(b, total):
        return jnp.where(lane == b, jnp.sum(squares[b]), total)

    packed = lax.fori_loop(
        0, embed_blocks + head_blocks, pack, jnp.zeros((8, LANES), jnp.float32)
    )
    mine[...] = packed
    column_sums[me] = packed

    tail_copy.start()

    for k in near:
        send(k, 0, bulk).wait_send()
    send(1, 0, bulk).start()

    def stat_copy(k):
        return pltpu.make_async_remote_copy(
            src_ref=mine,
            dst_ref=column_sums.at[me],
            send_sem=stat_send.at[k],
            recv_sem=stat_recv.at[k],
            device_id={"mp": partner(me, k, pieces)},
            device_id_type=MESH,
        )

    for k in range(1, pieces):
        stat_copy(k).start()
    send(first_late, half, bulk - half).start()
    for k in late[1:]:
        send(k, 0, bulk).start()
    for k in range(1, pieces):
        stat_copy(k).wait()
    packed = jnp.sum(column_sums[...], axis=0)
    shard_mine[...] = packed
    shard_sums[shard] = packed

    def shard_copy(k):
        return pltpu.make_async_remote_copy(
            src_ref=shard_mine,
            dst_ref=shard_sums.at[shard],
            send_sem=shard_send.at[k],
            recv_sem=shard_recv.at[k],
            device_id={"dp": partner(shard, k, shards)},
            device_id_type=MESH,
        )

    for k in range(1, shards):
        shard_copy(k).start()
    for k in range(1, shards):
        shard_copy(k).wait()
    sums[...] = shard_sums[...]

    own_copy.wait()
    tail_copy.wait()
    for k in range(1, pieces):
        if k not in near:
            send(k, 0, bulk).wait_send()
        send(k, 0, bulk).wait_recv()


def round_and_exchange(by_owner, mtp, shards, tiles, tail_tiles):
    pieces, rows, width = by_owner.shape
    tile = rows // tiles
    bulk_rows, tail_rows = (tiles - tail_tiles) * tile, tail_tiles * tile
    blocks = pieces * rows // EMB_BLK + mtp.shape[0] // MTP_BLK
    return pl.pallas_call(
        functools.partial(exchange_kernel, pieces, shards, tiles, tail_tiles),
        in_specs=[pl.BlockSpec(memory_space=pl.ANY)] * 2,
        out_specs=[
            pl.BlockSpec(memory_space=pl.ANY),
            pl.BlockSpec(memory_space=pl.ANY),
            pl.BlockSpec(memory_space=pltpu.VMEM),
        ],
        out_shape=[
            jax.ShapeDtypeStruct((pieces, bulk_rows, width), jnp.bfloat16),
            jax.ShapeDtypeStruct((pieces, tail_rows, width), jnp.bfloat16),
            jax.ShapeDtypeStruct((shards, 8, LANES), jnp.float32),
        ],
        scratch_shapes=[
            pltpu.VMEM((pieces, bulk_rows, width), jnp.bfloat16),
            pltpu.VMEM((pieces, tail_rows, width), jnp.bfloat16),
            pltpu.VMEM((SLOTS, tile, width), jnp.float32),
            pltpu.VMEM((2, MTP_BLK, width), jnp.float32),
            pltpu.VMEM((blocks, 8, width), jnp.float32),
            pltpu.VMEM((8, LANES), jnp.float32),
            pltpu.VMEM((pieces, 8, LANES), jnp.float32),
            pltpu.VMEM((8, LANES), jnp.float32),
            pltpu.VMEM((shards, 8, LANES), jnp.float32),
            pltpu.SemaphoreType.DMA((SLOTS,)),
            pltpu.SemaphoreType.DMA((2,)),
            pltpu.SemaphoreType.DMA((pieces,)),
            pltpu.SemaphoreType.DMA((pieces,)),
            pltpu.SemaphoreType.DMA,
            pltpu.SemaphoreType.DMA,
            pltpu.SemaphoreType.DMA((pieces,)),
            pltpu.SemaphoreType.DMA((pieces,)),
            pltpu.SemaphoreType.DMA((shards,)),
            pltpu.SemaphoreType.DMA((shards,)),
        ],
        compiler_params=pltpu.CompilerParams(
            collective_id=0, has_side_effects=True, vmem_limit_bytes=60_000_000
        ),
        cost_estimate=pl.CostEstimate(
            flops=3 * by_owner.size, bytes_accessed=8 * by_owner.size, transcendentals=0
        ),
    )(by_owner, mtp)


def scale_kernel(factor_ref, x_ref, out_ref):
    pieces, _, width = x_ref.shape
    factor = factor_ref[0]
    for j in range(pieces):
        out_ref[:, j * width : (j + 1) * width] = (
            x_ref[j].astype(jnp.float32) * factor
        ).astype(jnp.bfloat16)


def scale_rows(factor, arrived, rows, tile):
    pieces, count, width = arrived.shape
    return pl.pallas_call(
        scale_kernel,
        grid=(count // tile,),
        in_specs=[
            pl.BlockSpec(memory_space=pltpu.SMEM),
            pl.BlockSpec((pieces, tile, width), lambda i: (0, i, 0)),
        ],
        out_specs=pl.BlockSpec((tile, pieces * width), lambda i: (i, 0)),
        out_shape=jax.ShapeDtypeStruct((rows, pieces * width), jnp.bfloat16),
        cost_estimate=pl.CostEstimate(
            flops=arrived.size, bytes_accessed=4 * arrived.size, transcendentals=0
        ),
    )(factor.reshape(1), arrived)


def scale_tail_kernel(step, factor_ref, x_ref, _, out_ref):
    pieces, _, width = x_ref.shape
    factor = factor_ref[0]
    at = pl.ds(pl.multiple_of(pl.program_id(0) * step, step), step)
    for j in range(pieces):
        out_ref[:, j * width : (j + 1) * width] = (
            x_ref[j, at, :].astype(jnp.float32) * factor
        ).astype(jnp.bfloat16)


def scale_tail(factor, arrived, out, step):
    pieces, count, width = arrived.shape
    start = (out.shape[0] - count) // step
    return pl.pallas_call(
        functools.partial(scale_tail_kernel, step),
        grid=(count // step,),
        in_specs=[
            pl.BlockSpec(memory_space=pltpu.SMEM),
            pl.BlockSpec(memory_space=pltpu.VMEM),
            pl.BlockSpec(memory_space=pl.ANY),
        ],
        out_specs=pl.BlockSpec((step, pieces * width), lambda i: (start + i, 0)),
        out_shape=jax.ShapeDtypeStruct(out.shape, jnp.bfloat16),
        input_output_aliases={2: 0},
        compiler_params=pltpu.CompilerParams(vmem_limit_bytes=16 * step * pieces * width),
        cost_estimate=pl.CostEstimate(
            flops=arrived.size, bytes_accessed=4 * arrived.size, transcendentals=0
        ),
    )(factor.reshape(1), arrived, out)


def membership(labels):
    return (labels[:, None] == jnp.arange(GROUPS, dtype=jnp.int32)[None, :]).astype(jnp.float32)


def on_device(shards, pieces, emb_grad, mtp_grad, emb_groups, mtp_groups, max_rms):
    width = emb_grad.shape[1]
    model_width = width * pieces
    total_rows = (emb_grad.shape[0] + mtp_grad.shape[0]) * shards
    rows = emb_grad.shape[0] // pieces
    tiles, tail_tiles = 16, 1
    tile = rows // tiles

    by_owner = emb_grad.reshape(pieces, rows, width)
    arrived, tail, sums = round_and_exchange(by_owner, mtp_grad, shards, tiles, tail_tiles)
    tail_arrived = lax.all_to_all(tail, "mp", split_axis=0, concat_axis=0, tiled=True)

    embed_count = emb_grad.shape[0] // EMB_BLK
    head_count = mtp_grad.shape[0] // MTP_BLK
    flat = sums.reshape(shards, 8 * LANES)
    embed_squares = flat[:, :embed_count].reshape(-1)
    head_squares = flat[:, embed_count : embed_count + head_count].reshape(-1)
    embed_member, head_member = membership(emb_groups), membership(mtp_groups)
    group_square = jnp.sum(embed_squares[:, None] * embed_member, axis=0) + jnp.sum(
        head_squares[:, None] * head_member, axis=0
    )
    group_size = jnp.sum(embed_member, axis=0) * jnp.float32(
        EMB_BLK * model_width
    ) + jnp.sum(head_member, axis=0) * jnp.float32(MTP_BLK * model_width)
    group_rms = jnp.sqrt(group_square / jnp.maximum(group_size, 1.0))
    global_norm = jnp.sqrt(jnp.sum(group_square))
    ceiling = max_rms[0] * jnp.sqrt(jnp.float32(total_rows * model_width))
    factor = ceiling / (global_norm + 1e-06)
    out = scale_rows(factor, arrived, rows, tile)
    head_output = (mtp_grad * factor).astype(jnp.bfloat16)
    out = scale_tail(factor, tail_arrived, out, tile // 4)
    return (out, head_output, group_rms)


def solution(mesh):
    placed = (P("dp", "mp"), P("dp", "mp"), P(), P(), P())
    return jax.shard_map(
        functools.partial(on_device, mesh.shape["dp"], mesh.shape["mp"]),
        mesh=mesh,
        in_specs=placed,
        out_specs=(P(("dp", "mp"), None), P("dp", "mp"), P()),
        check_vma=False,
    )
```

```python
import functools

import jax
import jax.numpy as jnp
from jax import lax
from jax.experimental import pallas as pl
from jax.experimental.pallas import tpu as pltpu
from jax.sharding import PartitionSpec as P

EMB_BLK = 1024
MTP_BLK = 448
GROUPS = 32
STRIP = 32
SLOTS = 6
LEAD = 2
TILES = 16
TAIL_TILES = 4
LANES = 128
MESH = pl.DeviceIdType.MESH


def partner(me, k, count):
    out, bit = 0, 1
    while bit < count:
        mine, other = (me // bit) % 2, (k // bit) % 2
        out = out + bit * (mine + other - 2 * mine * other)
        bit *= 2
    return out


def exchange_kernel(
    pieces, shards, tiles, tail_tiles,
    emb, mtp, arrived, tail_out, sums,
    low, slots, head_slots, squares, mine, column_sums, shard_mine, shard_sums,
    load_sem, head_sem, send_sem, recv_sem, own_sem, tail_sem,
    stat_send, stat_recv, shard_send, shard_recv,
):
    me, shard = lax.axis_index("mp"), lax.axis_index("dp")
    _, rows, width = emb.shape
    tile = slots.shape[1]
    embed_blocks = pieces * rows // EMB_BLK
    head_blocks = mtp.shape[0] // MTP_BLK
    middle = pieces // 2
    bulk = tiles - tail_tiles

    def sent(k):
        return bulk if k == middle else tiles

    barrier = pltpu.get_barrier_semaphore()
    for k in range(1, pieces):
        pl.semaphore_signal(
            barrier, inc=1, device_id={"mp": partner(me, k, pieces)}, device_id_type=MESH
        )
    for k in range(1, shards):
        pl.semaphore_signal(
            barrier, inc=1, device_id={"dp": partner(shard, k, shards)}, device_id_type=MESH
        )

    def stream(count, place, store, after):
        def load(i):
            piece, t = place(i)
            return pltpu.make_async_copy(
                emb.at[piece, pl.ds(pl.multiple_of(t * tile, tile), tile), :],
                slots.at[i % SLOTS],
                load_sem.at[i % SLOTS],
            )

        def prime():
            for i in range(min(SLOTS, count)):
                load(i).start()

        def run():
            @pl.loop(0, count)
            def _(i):
                load(i).wait()
                piece, t = place(i)
                block = (piece * rows + t * tile) // EMB_BLK
                slot = i % SLOTS

                def strip(j, total):
                    at = pl.multiple_of(j * STRIP, STRIP)
                    x = slots[slot, pl.ds(at, STRIP), :]
                    store(i, at, x.astype(jnp.bfloat16))
                    return total + jnp.sum((x * x).reshape(STRIP // 8, 8, width), axis=0)

                total = lax.fori_loop(
                    0, tile // STRIP, strip, jnp.zeros((8, width), jnp.float32)
                )
                squares[block] = squares[block] + total

                @pl.when(i + SLOTS < count)
                def _():
                    load(i + SLOTS).start()

                @pl.when(i > 0)
                def _():
                    after(i - 1)

            after(count - 1)

        return prime, run

    def store_low(k, t, at, value):
        low[k, pl.ds(pl.multiple_of(t * tile + at, STRIP), STRIP), :] = value

    def send(k, start, count):
        at = pl.ds(pl.multiple_of(start * tile, tile), count * tile)
        return pltpu.make_async_remote_copy(
            src_ref=low.at[k, at, :],
            dst_ref=arrived.at[me, at, :],
            send_sem=send_sem.at[k],
            recv_sem=recv_sem.at[k],
            device_id={"mp": partner(me, k, pieces)},
            device_id_type=MESH,
        )

    near = list(range(2, middle))
    early = list(range(pieces - 1, middle + middle // 2 - 1, -1))
    late = list(range(middle + middle // 2 - 1, middle - 1, -1))
    lead = min(LEAD, bulk - 1)
    paired = min(len(near), len(early))

    def lead_piece(i):
        pair = (i // 2) % paired
        return (1 - i % 2) * (2 + pair) + (i % 2) * (pieces - 1 - pair)

    def lead_tile(i):
        return i // (2 * paired)

    prime, run = stream(
        2 * paired * lead,
        lambda i: (partner(me, lead_piece(i), pieces), lead_tile(i)),
        lambda i, at, value: store_low(lead_piece(i), lead_tile(i), at, value),
        lambda i: None,
    )
    prime()
    squares[...] = jnp.zeros_like(squares)
    run()
    pl.semaphore_wait(barrier, pieces - 1 + shards - 1)
    for pair in range(paired):
        send(near[pair], 0, lead).start()
        send(early[pair], 0, lead).start()

    waiting = []
    for k in near + early + late + [1]:
        started = lead if k in near[:paired] + early[:paired] else 0
        prime, run = stream(
            tiles - started,
            lambda i: (partner(me, k, pieces), started + i),
            lambda i, at, value: store_low(k, started + i, at, value),
            lambda i: None,
        )
        prime()
        run()
        for copy in waiting:
            copy.start()
        waiting = [send(k, started, tiles - started)] if k in near + early else []
    first_late = late[0]
    half = tiles // 2

    own_copy = pltpu.make_async_copy(low.at[0], arrived.at[me], own_sem)
    tail_copy = pltpu.make_async_copy(
        low.at[middle, pl.ds(bulk * tile, tail_tiles * tile), :], tail_out, tail_sem
    )
    prime, run = stream(
        tiles,
        lambda i: (me, i),
        lambda i, at, value: store_low(0, i, at, value),
        lambda i: None,
    )
    prime()
    run()
    send(first_late, 0, half).start()

    tail_copy.start()
    own_copy.start()

    def head_load(b):
        return pltpu.make_async_copy(
            mtp.at[pl.ds(pl.multiple_of(b * MTP_BLK, MTP_BLK), MTP_BLK), :],
            head_slots.at[b % 2],
            head_sem.at[b % 2],
        )

    for b in range(min(2, head_blocks)):
        head_load(b).start()

    @pl.loop(0, head_blocks)
    def _(b):
        head_load(b).wait()

        def strip(j, total):
            x = head_slots[b % 2, pl.ds(pl.multiple_of(j * STRIP, STRIP), STRIP), :]
            return total + jnp.sum((x * x).reshape(STRIP // 8, 8, width), axis=0)

        squares[embed_blocks + b] = lax.fori_loop(
            0, MTP_BLK // STRIP, strip, jnp.zeros((8, width), jnp.float32)
        )

        @pl.when(b + 2 < head_blocks)
        def _():
            head_load(b + 2).start()

    lane = lax.broadcasted_iota(jnp.int32, (8, LANES), 0) * LANES + lax.broadcasted_iota(
        jnp.int32, (8, LANES), 1
    )

    def pack(b, total):
        return jnp.where(lane == b, jnp.sum(squares[b]), total)

    packed = lax.fori_loop(
        0, embed_blocks + head_blocks, pack, jnp.zeros((8, LANES), jnp.float32)
    )
    mine[...] = packed
    column_sums[me] = packed

    for k in near:
        send(k, 0, tiles).wait_send()
    send(1, 0, tiles).start()

    def stat_copy(k):
        return pltpu.make_async_remote_copy(
            src_ref=mine,
            dst_ref=column_sums.at[me],
            send_sem=stat_send.at[k],
            recv_sem=stat_recv.at[k],
            device_id={"mp": partner(me, k, pieces)},
            device_id_type=MESH,
        )

    for k in range(1, pieces):
        stat_copy(k).start()
    send(first_late, half, tiles - half).start()
    for k in late[1:]:
        send(k, 0, sent(k)).start()
    for k in range(1, pieces):
        stat_copy(k).wait()
    packed = jnp.sum(column_sums[...], axis=0)
    shard_mine[...] = packed
    shard_sums[shard] = packed

    def shard_copy(k):
        return pltpu.make_async_remote_copy(
            src_ref=shard_mine,
            dst_ref=shard_sums.at[shard],
            send_sem=shard_send.at[k],
            recv_sem=shard_recv.at[k],
            device_id={"dp": partner(shard, k, shards)},
            device_id_type=MESH,
        )

    for k in range(1, shards):
        shard_copy(k).start()
    for k in range(1, shards):
        shard_copy(k).wait()
    sums[...] = shard_sums[...]

    own_copy.wait()
    tail_copy.wait()
    for k in range(1, pieces):
        if k not in near:
            send(k, 0, sent(k)).wait_send()
        send(k, 0, sent(k)).wait_recv()


def round_and_exchange(by_owner, mtp, shards, tiles, tail_tiles):
    pieces, rows, width = by_owner.shape
    tile = rows // tiles
    blocks = pieces * rows // EMB_BLK + mtp.shape[0] // MTP_BLK
    return pl.pallas_call(
        functools.partial(exchange_kernel, pieces, shards, tiles, tail_tiles),
        in_specs=[pl.BlockSpec(memory_space=pl.ANY)] * 2,
        out_specs=[
            pl.BlockSpec(memory_space=pl.ANY),
            pl.BlockSpec(memory_space=pl.ANY),
            pl.BlockSpec(memory_space=pltpu.VMEM),
        ],
        out_shape=[
            jax.ShapeDtypeStruct(by_owner.shape, jnp.bfloat16),
            jax.ShapeDtypeStruct((tail_tiles * tile, width), jnp.bfloat16),
            jax.ShapeDtypeStruct((shards, 8, LANES), jnp.float32),
        ],
        scratch_shapes=[
            pltpu.VMEM(by_owner.shape, jnp.bfloat16),
            pltpu.VMEM((SLOTS, tile, width), jnp.float32),
            pltpu.VMEM((2, MTP_BLK, width), jnp.float32),
            pltpu.VMEM((blocks, 8, width), jnp.float32),
            pltpu.VMEM((8, LANES), jnp.float32),
            pltpu.VMEM((pieces, 8, LANES), jnp.float32),
            pltpu.VMEM((8, LANES), jnp.float32),
            pltpu.VMEM((shards, 8, LANES), jnp.float32),
            pltpu.SemaphoreType.DMA((SLOTS,)),
            pltpu.SemaphoreType.DMA((2,)),
            pltpu.SemaphoreType.DMA((pieces,)),
            pltpu.SemaphoreType.DMA((pieces,)),
            pltpu.SemaphoreType.DMA,
            pltpu.SemaphoreType.DMA,
            pltpu.SemaphoreType.DMA((pieces,)),
            pltpu.SemaphoreType.DMA((pieces,)),
            pltpu.SemaphoreType.DMA((shards,)),
            pltpu.SemaphoreType.DMA((shards,)),
        ],
        compiler_params=pltpu.CompilerParams(
            collective_id=0, has_side_effects=True, vmem_limit_bytes=60_000_000
        ),
        cost_estimate=pl.CostEstimate(
            flops=3 * by_owner.size, bytes_accessed=8 * by_owner.size, transcendentals=0
        ),
    )(by_owner, mtp)


def scale_kernel(factor_ref, x_ref, out_ref):
    pieces, _, width = x_ref.shape
    factor = factor_ref[0]
    for j in range(pieces):
        out_ref[:, j * width : (j + 1) * width] = (
            x_ref[j].astype(jnp.float32) * factor
        ).astype(jnp.bfloat16)


def scale_rows(factor, arrived, rows, tile):
    pieces, count, width = arrived.shape
    return pl.pallas_call(
        scale_kernel,
        grid=(count // tile,),
        in_specs=[
            pl.BlockSpec(memory_space=pltpu.SMEM),
            pl.BlockSpec((pieces, tile, width), lambda i: (0, i, 0)),
        ],
        out_specs=pl.BlockSpec((tile, pieces * width), lambda i: (i, 0)),
        out_shape=jax.ShapeDtypeStruct((rows, pieces * width), jnp.bfloat16),
        cost_estimate=pl.CostEstimate(
            flops=arrived.size, bytes_accessed=4 * arrived.size, transcendentals=0
        ),
    )(factor.reshape(1), arrived)


def scale_tail_kernel(step, _, factor_ref, x_ref, __, out_ref):
    at = pl.ds(pl.multiple_of(pl.program_id(0) * step, step), step)
    out_ref[...] = (x_ref[at, :].astype(jnp.float32) * factor_ref[0]).astype(jnp.bfloat16)


def scale_tail(factor, piece, arrived, out, step):
    count, width = arrived.shape
    start = (out.shape[0] - count) // step
    if width % LANES:
        scaled = (arrived.astype(jnp.float32) * factor).astype(jnp.bfloat16)
        return lax.dynamic_update_slice(out, scaled, (out.shape[0] - count, piece * width))
    return pl.pallas_call(
        functools.partial(scale_tail_kernel, step),
        grid_spec=pltpu.PrefetchScalarGridSpec(
            num_scalar_prefetch=1,
            grid=(count // step,),
            in_specs=[
                pl.BlockSpec(memory_space=pltpu.SMEM),
                pl.BlockSpec(memory_space=pltpu.VMEM),
                pl.BlockSpec(memory_space=pl.ANY),
            ],
            out_specs=pl.BlockSpec((step, width), lambda i, piece: (start + i, piece[0])),
        ),
        out_shape=jax.ShapeDtypeStruct(out.shape, jnp.bfloat16),
        input_output_aliases={3: 0},
        compiler_params=pltpu.CompilerParams(vmem_limit_bytes=32 * step * width),
        cost_estimate=pl.CostEstimate(
            flops=arrived.size, bytes_accessed=4 * arrived.size, transcendentals=0
        ),
    )(piece.reshape(1), factor.reshape(1), arrived, out)


def membership(labels):
    return (labels[:, None] == jnp.arange(GROUPS, dtype=jnp.int32)[None, :]).astype(jnp.float32)


def on_device(shards, pieces, emb_grad, mtp_grad, emb_groups, mtp_groups, max_rms):
    width = emb_grad.shape[1]
    model_width = width * pieces
    total_rows = (emb_grad.shape[0] + mtp_grad.shape[0]) * shards
    rows = emb_grad.shape[0] // pieces
    tiles, tail_tiles = TILES, TAIL_TILES
    tile = rows // tiles

    by_owner = emb_grad.reshape(pieces, rows, width)
    arrived, tail, sums = round_and_exchange(by_owner, mtp_grad, shards, tiles, tail_tiles)
    middle = pieces // 2
    tail_arrived = lax.ppermute(tail, "mp", [(i, (i + middle) % pieces) for i in range(pieces)])
    source = (lax.axis_index("mp") + middle) % pieces

    embed_count = emb_grad.shape[0] // EMB_BLK
    head_count = mtp_grad.shape[0] // MTP_BLK
    flat = sums.reshape(shards, 8 * LANES)
    embed_squares = flat[:, :embed_count].reshape(-1)
    head_squares = flat[:, embed_count : embed_count + head_count].reshape(-1)
    embed_member, head_member = membership(emb_groups), membership(mtp_groups)
    group_square = jnp.sum(embed_squares[:, None] * embed_member, axis=0) + jnp.sum(
        head_squares[:, None] * head_member, axis=0
    )
    group_size = jnp.sum(embed_member, axis=0) * jnp.float32(
        EMB_BLK * model_width
    ) + jnp.sum(head_member, axis=0) * jnp.float32(MTP_BLK * model_width)
    group_rms = jnp.sqrt(group_square / jnp.maximum(group_size, 1.0))
    global_norm = jnp.sqrt(jnp.sum(group_square))
    ceiling = max_rms[0] * jnp.sqrt(jnp.float32(total_rows * model_width))
    factor = ceiling / (global_norm + 1e-06)
    out = scale_rows(factor, arrived, rows, tile)
    head_output = (mtp_grad * factor).astype(jnp.bfloat16)
    out = scale_tail(factor, source, tail_arrived, out, tile)
    return (out, head_output, group_rms)


def solution(mesh):
    placed = (P("dp", "mp"), P("dp", "mp"), P(), P(), P())
    return jax.shard_map(
        functools.partial(on_device, mesh.shape["dp"], mesh.shape["mp"]),
        mesh=mesh,
        in_specs=placed,
        out_specs=(P(("dp", "mp"), None), P("dp", "mp"), P()),
        check_vma=False,
    )
```

```python
import functools

import jax
import jax.numpy as jnp
from jax import lax
from jax.experimental import pallas as pl
from jax.experimental.pallas import tpu as pltpu
from jax.sharding import PartitionSpec as P

EMB_BLK = 1024
MTP_BLK = 448
GROUPS = 32
STRIP = 32
SLOTS = 6
LEAD = 2
TILES = 16
TAIL_TILES = 4
LANES = 128
MESH = pl.DeviceIdType.MESH


def partner(me, k, count):
    out, bit = 0, 1
    while bit < count:
        mine, other = (me // bit) % 2, (k // bit) % 2
        out = out + bit * (mine + other - 2 * mine * other)
        bit *= 2
    return out


def exchange_kernel(
    pieces, shards, tiles, tail_tiles,
    emb, mtp, arrived, tail_out, sums,
    low, slots, head_slots, squares, mine, column_sums, shard_mine, shard_sums,
    load_sem, head_sem, send_sem, recv_sem, own_sem, tail_sem,
    stat_send, stat_recv, shard_send, shard_recv,
):
    me, shard = lax.axis_index("mp"), lax.axis_index("dp")
    _, rows, width = emb.shape
    tile = slots.shape[1]
    embed_blocks = pieces * rows // EMB_BLK
    head_blocks = mtp.shape[0] // MTP_BLK
    middle = pieces // 2
    held = pieces - 2
    bulk = tiles - tail_tiles

    def sent(k):
        return bulk if k == held else tiles

    barrier = pltpu.get_barrier_semaphore()
    for k in range(1, pieces):
        pl.semaphore_signal(
            barrier, inc=1, device_id={"mp": partner(me, k, pieces)}, device_id_type=MESH
        )
    for k in range(1, shards):
        pl.semaphore_signal(
            barrier, inc=1, device_id={"dp": partner(shard, k, shards)}, device_id_type=MESH
        )

    def stream(count, place, store, after):
        def load(i):
            piece, t = place(i)
            return pltpu.make_async_copy(
                emb.at[piece, pl.ds(pl.multiple_of(t * tile, tile), tile), :],
                slots.at[i % SLOTS],
                load_sem.at[i % SLOTS],
            )

        def prime():
            for i in range(min(SLOTS, count)):
                load(i).start()

        def run():
            @pl.loop(0, count)
            def _(i):
                load(i).wait()
                piece, t = place(i)
                block = (piece * rows + t * tile) // EMB_BLK
                slot = i % SLOTS

                def strip(j, total):
                    at = pl.multiple_of(j * STRIP, STRIP)
                    x = slots[slot, pl.ds(at, STRIP), :]
                    store(i, at, x.astype(jnp.bfloat16))
                    return total + jnp.sum((x * x).reshape(STRIP // 8, 8, width), axis=0)

                total = lax.fori_loop(
                    0, tile // STRIP, strip, jnp.zeros((8, width), jnp.float32)
                )
                squares[block] = squares[block] + total

                @pl.when(i + SLOTS < count)
                def _():
                    load(i + SLOTS).start()

                @pl.when(i > 0)
                def _():
                    after(i - 1)

            after(count - 1)

        return prime, run

    def store_low(k, t, at, value):
        low[k, pl.ds(pl.multiple_of(t * tile + at, STRIP), STRIP), :] = value

    def send(k, start, count):
        at = pl.ds(pl.multiple_of(start * tile, tile), count * tile)
        return pltpu.make_async_remote_copy(
            src_ref=low.at[k, at, :],
            dst_ref=arrived.at[me, at, :],
            send_sem=send_sem.at[k],
            recv_sem=recv_sem.at[k],
            device_id={"mp": partner(me, k, pieces)},
            device_id_type=MESH,
        )

    near = list(range(middle - 1, 1, -1))
    early = [held, pieces - 1] + list(range(middle + middle // 2, held))
    late = list(range(middle + middle // 2 - 1, middle - 1, -1))
    lead = min(LEAD, bulk - 1)
    paired = 2

    def lead_piece(i):
        pair = (i // 2) % paired
        near_piece, early_piece = middle - 1 - pair, held + pair
        return (1 - i % 2) * near_piece + (i % 2) * early_piece

    def lead_tile(i):
        return i // (2 * paired)

    prime, run = stream(
        2 * paired * lead,
        lambda i: (partner(me, lead_piece(i), pieces), lead_tile(i)),
        lambda i, at, value: store_low(lead_piece(i), lead_tile(i), at, value),
        lambda i: None,
    )
    prime()
    squares[...] = jnp.zeros_like(squares)
    run()
    pl.semaphore_wait(barrier, pieces - 1 + shards - 1)
    for pair in range(paired):
        send(near[pair], 0, lead).start()
        send(early[pair], 0, lead).start()

    inner = ((me // (pieces // 4) + 1) // 2) % 2
    split_send = send(near[0], bulk, tiles - bulk)
    waiting, waiting_split = [], False
    for k in near + early + late + [1]:
        started = lead if k in near[:paired] + early[:paired] else 0
        prime, run = stream(
            tiles - started,
            lambda i: (partner(me, k, pieces), started + i),
            lambda i, at, value: store_low(k, started + i, at, value),
            lambda i: None,
        )
        prime()
        run()
        for copy in waiting:
            copy.start()
        if waiting_split:
            waiting_split = False

            @pl.when(inner == 0)
            def _():
                split_send.start()

        if k == near[-1]:
            waiting = [send(k, started, tiles - started)]
            waiting_split = True
        elif k in near + early:
            stop = bulk if k in (near[0], held) else tiles
            waiting = [send(k, started, stop - started)]
        else:
            waiting = []
    first_late = late[0]
    half = tiles // 2

    own_copy = pltpu.make_async_copy(low.at[0], arrived.at[me], own_sem)
    tail_copy = pltpu.make_async_copy(
        low.at[held, pl.ds(bulk * tile, tail_tiles * tile), :], tail_out, tail_sem
    )
    prime, run = stream(
        tiles,
        lambda i: (me, i),
        lambda i, at, value: store_low(0, i, at, value),
        lambda i: None,
    )
    prime()
    run()
    send(first_late, 0, half).start()

    tail_copy.start()
    own_copy.start()

    def head_load(b):
        return pltpu.make_async_copy(
            mtp.at[pl.ds(pl.multiple_of(b * MTP_BLK, MTP_BLK), MTP_BLK), :],
            head_slots.at[b % 2],
            head_sem.at[b % 2],
        )

    for b in range(min(2, head_blocks)):
        head_load(b).start()

    @pl.loop(0, head_blocks)
    def _(b):
        head_load(b).wait()

        def strip(j, total):
            x = head_slots[b % 2, pl.ds(pl.multiple_of(j * STRIP, STRIP), STRIP), :]
            return total + jnp.sum((x * x).reshape(STRIP // 8, 8, width), axis=0)

        squares[embed_blocks + b] = lax.fori_loop(
            0, MTP_BLK // STRIP, strip, jnp.zeros((8, width), jnp.float32)
        )

        @pl.when(b + 2 < head_blocks)
        def _():
            head_load(b + 2).start()

    lane = lax.broadcasted_iota(jnp.int32, (8, LANES), 0) * LANES + lax.broadcasted_iota(
        jnp.int32, (8, LANES), 1
    )

    def pack(b, total):
        return jnp.where(lane == b, jnp.sum(squares[b]), total)

    packed = lax.fori_loop(
        0, embed_blocks + head_blocks, pack, jnp.zeros((8, LANES), jnp.float32)
    )
    mine[...] = packed
    column_sums[me] = packed

    for k in near[1:]:
        send(k, 0, tiles).wait_send()
    send(1, 0, tiles).start()

    @pl.when(inner == 1)
    def _():
        split_send.start()

    def stat_copy(k):
        return pltpu.make_async_remote_copy(
            src_ref=mine,
            dst_ref=column_sums.at[me],
            send_sem=stat_send.at[k],
            recv_sem=stat_recv.at[k],
            device_id={"mp": partner(me, k, pieces)},
            device_id_type=MESH,
        )

    for k in range(1, pieces):
        stat_copy(k).start()
    send(first_late, half, tiles - half).start()
    for k in late[1:]:
        send(k, 0, sent(k)).start()
    for k in range(1, pieces):
        stat_copy(k).wait()
    packed = jnp.sum(column_sums[...], axis=0)
    shard_mine[...] = packed
    shard_sums[shard] = packed

    def shard_copy(k):
        return pltpu.make_async_remote_copy(
            src_ref=shard_mine,
            dst_ref=shard_sums.at[shard],
            send_sem=shard_send.at[k],
            recv_sem=shard_recv.at[k],
            device_id={"dp": partner(shard, k, shards)},
            device_id_type=MESH,
        )

    for k in range(1, shards):
        shard_copy(k).start()
    for k in range(1, shards):
        shard_copy(k).wait()
    sums[...] = shard_sums[...]

    own_copy.wait()
    tail_copy.wait()
    for k in range(1, pieces):
        if k not in near[1:]:
            send(k, 0, sent(k)).wait_send()
        send(k, 0, sent(k)).wait_recv()


def round_and_exchange(by_owner, mtp, shards, tiles, tail_tiles):
    pieces, rows, width = by_owner.shape
    tile = rows // tiles
    blocks = pieces * rows // EMB_BLK + mtp.shape[0] // MTP_BLK
    return pl.pallas_call(
        functools.partial(exchange_kernel, pieces, shards, tiles, tail_tiles),
        in_specs=[pl.BlockSpec(memory_space=pl.ANY)] * 2,
        out_specs=[
            pl.BlockSpec(memory_space=pl.ANY),
            pl.BlockSpec(memory_space=pl.ANY),
            pl.BlockSpec(memory_space=pltpu.VMEM),
        ],
        out_shape=[
            jax.ShapeDtypeStruct(by_owner.shape, jnp.bfloat16),
            jax.ShapeDtypeStruct((tail_tiles * tile, width), jnp.bfloat16),
            jax.ShapeDtypeStruct((shards, 8, LANES), jnp.float32),
        ],
        scratch_shapes=[
            pltpu.VMEM(by_owner.shape, jnp.bfloat16),
            pltpu.VMEM((SLOTS, tile, width), jnp.float32),
            pltpu.VMEM((2, MTP_BLK, width), jnp.float32),
            pltpu.VMEM((blocks, 8, width), jnp.float32),
            pltpu.VMEM((8, LANES), jnp.float32),
            pltpu.VMEM((pieces, 8, LANES), jnp.float32),
            pltpu.VMEM((8, LANES), jnp.float32),
            pltpu.VMEM((shards, 8, LANES), jnp.float32),
            pltpu.SemaphoreType.DMA((SLOTS,)),
            pltpu.SemaphoreType.DMA((2,)),
            pltpu.SemaphoreType.DMA((pieces,)),
            pltpu.SemaphoreType.DMA((pieces,)),
            pltpu.SemaphoreType.DMA,
            pltpu.SemaphoreType.DMA,
            pltpu.SemaphoreType.DMA((pieces,)),
            pltpu.SemaphoreType.DMA((pieces,)),
            pltpu.SemaphoreType.DMA((shards,)),
            pltpu.SemaphoreType.DMA((shards,)),
        ],
        compiler_params=pltpu.CompilerParams(
            collective_id=0, has_side_effects=True, vmem_limit_bytes=60_000_000
        ),
        cost_estimate=pl.CostEstimate(
            flops=3 * by_owner.size, bytes_accessed=8 * by_owner.size, transcendentals=0
        ),
    )(by_owner, mtp)


def scale_kernel(factor_ref, x_ref, out_ref):
    pieces, _, width = x_ref.shape
    factor = factor_ref[0]
    for j in range(pieces):
        out_ref[:, j * width : (j + 1) * width] = (
            x_ref[j].astype(jnp.float32) * factor
        ).astype(jnp.bfloat16)


def scale_rows(factor, arrived, rows, tile):
    pieces, count, width = arrived.shape
    return pl.pallas_call(
        scale_kernel,
        grid=(count // tile,),
        in_specs=[
            pl.BlockSpec(memory_space=pltpu.SMEM),
            pl.BlockSpec((pieces, tile, width), lambda i: (0, i, 0)),
        ],
        out_specs=pl.BlockSpec((tile, pieces * width), lambda i: (i, 0)),
        out_shape=jax.ShapeDtypeStruct((rows, pieces * width), jnp.bfloat16),
        cost_estimate=pl.CostEstimate(
            flops=arrived.size, bytes_accessed=4 * arrived.size, transcendentals=0
        ),
    )(factor.reshape(1), arrived)


def scale_tail_kernel(step, _, factor_ref, x_ref, __, out_ref):
    at = pl.ds(pl.multiple_of(pl.program_id(0) * step, step), step)
    out_ref[...] = (x_ref[at, :].astype(jnp.float32) * factor_ref[0]).astype(jnp.bfloat16)


def scale_tail(factor, piece, arrived, out, step):
    count, width = arrived.shape
    start = (out.shape[0] - count) // step
    if width % LANES:
        scaled = (arrived.astype(jnp.float32) * factor).astype(jnp.bfloat16)
        return lax.dynamic_update_slice(out, scaled, (out.shape[0] - count, piece * width))
    return pl.pallas_call(
        functools.partial(scale_tail_kernel, step),
        grid_spec=pltpu.PrefetchScalarGridSpec(
            num_scalar_prefetch=1,
            grid=(count // step,),
            in_specs=[
                pl.BlockSpec(memory_space=pltpu.SMEM),
                pl.BlockSpec(memory_space=pltpu.VMEM),
                pl.BlockSpec(memory_space=pl.ANY),
            ],
            out_specs=pl.BlockSpec((step, width), lambda i, piece: (start + i, piece[0])),
        ),
        out_shape=jax.ShapeDtypeStruct(out.shape, jnp.bfloat16),
        input_output_aliases={3: 0},
        compiler_params=pltpu.CompilerParams(vmem_limit_bytes=32 * step * width),
        cost_estimate=pl.CostEstimate(
            flops=arrived.size, bytes_accessed=4 * arrived.size, transcendentals=0
        ),
    )(piece.reshape(1), factor.reshape(1), arrived, out)


def membership(labels):
    return (labels[:, None] == jnp.arange(GROUPS, dtype=jnp.int32)[None, :]).astype(jnp.float32)


def on_device(shards, pieces, emb_grad, mtp_grad, emb_groups, mtp_groups, max_rms):
    width = emb_grad.shape[1]
    model_width = width * pieces
    total_rows = (emb_grad.shape[0] + mtp_grad.shape[0]) * shards
    rows = emb_grad.shape[0] // pieces
    tiles, tail_tiles = TILES, TAIL_TILES
    tile = rows // tiles

    by_owner = emb_grad.reshape(pieces, rows, width)
    arrived, tail, sums = round_and_exchange(by_owner, mtp_grad, shards, tiles, tail_tiles)
    held = pieces - 2
    pairs = [(i, partner(i, held, pieces)) for i in range(pieces)]
    tail_arrived = lax.ppermute(tail, "mp", pairs)
    source = partner(lax.axis_index("mp"), held, pieces)

    embed_count = emb_grad.shape[0] // EMB_BLK
    head_count = mtp_grad.shape[0] // MTP_BLK
    flat = sums.reshape(shards, 8 * LANES)
    embed_squares = flat[:, :embed_count].reshape(-1)
    head_squares = flat[:, embed_count : embed_count + head_count].reshape(-1)
    embed_member, head_member = membership(emb_groups), membership(mtp_groups)
    group_square = jnp.sum(embed_squares[:, None] * embed_member, axis=0) + jnp.sum(
        head_squares[:, None] * head_member, axis=0
    )
    group_size = jnp.sum(embed_member, axis=0) * jnp.float32(
        EMB_BLK * model_width
    ) + jnp.sum(head_member, axis=0) * jnp.float32(MTP_BLK * model_width)
    group_rms = jnp.sqrt(group_square / jnp.maximum(group_size, 1.0))
    global_norm = jnp.sqrt(jnp.sum(group_square))
    ceiling = max_rms[0] * jnp.sqrt(jnp.float32(total_rows * model_width))
    factor = ceiling / (global_norm + 1e-06)
    out = scale_rows(factor, arrived, rows, 2 * tile)
    head_output = (mtp_grad * factor).astype(jnp.bfloat16)
    out = scale_tail(factor, source, tail_arrived, out, 2 * tile)
    return (out, head_output, group_rms)


def solution(mesh):
    placed = (P("dp", "mp"), P("dp", "mp"), P(), P(), P())
    return jax.shard_map(
        functools.partial(on_device, mesh.shape["dp"], mesh.shape["mp"]),
        mesh=mesh,
        in_specs=placed,
        out_specs=(P(("dp", "mp"), None), P("dp", "mp"), P()),
        check_vma=False,
    )
```
